32 devices in a mesh: row: 8 (over y, x, core), col: 4 (over z).
Axes of the slice: x: 2, y: 2, z: 4, core: 2. Of those that a mesh axis runs over, the one named last changes fastest.
Arguments:
- sources: float32 [8, 4, 512, 512], P('row', 'col'), may hold values from -6 to 6
- leaf_basis: float32 [8, 4, 512, 256], P('row', 'col'), may hold values from -0.25 to 0.25
- transfers: float32 [8, 4, 4, 256, 512], P('row', 'col'), may hold values from -0.25 to 0.25
- out_basis: float32 [8, 4, 512, 256], P('row', 'col'), may hold values from -0.375 to 0.375
Outputs:
- result: float32 [8, 4, 512, 512], P('row', 'col')
The draws below stay inside these ranges and needn't reach their ends.
All inputs are finite; a program needn't handle non-finite values.
Results may differ from the reference program's by a relative error of at most 0.0001.
Values sent between devices are 32-bit elements; how exact they have to be, the bound alone decides.
A program may use at most 64 MiB of HBM per device.

```python
import jax
import jax.numpy as jnp
from jax import lax

LEAF = 512
RANK = 256
RHS = 512
LEVELS = 4
N_ROW = 8
N_COL = 4


def levels(rng, dims, cuts, least, high):
    factor_of = 1.0
    for axis_at, blocks in cuts:
        draws = jax.random.uniform(jax.random.fold_in(jax.random.fold_in(rng, 6), axis_at), (blocks,), jnp.float32, least / len(cuts), high / len(cuts))
        factor_of = factor_of * jnp.repeat(jnp.exp(draws), dims[axis_at] // blocks).reshape((-1,) + (1,) * (len(dims) - 1 - axis_at))
    return factor_of


def gaussian(key, dims, deviation, limit, shards=(), held_as=jnp.bfloat16):
    drawn = deviation * jax.random.normal(key, dims, jnp.float32)
    if shards:
        drawn = drawn * levels(key, dims, shards, -0.22, 0.18)
    return jnp.clip(drawn, -limit, limit).astype(held_as)


def setup_inputs(seed: int = 0) -> dict:
    seeds = jax.random.split(jax.random.key(seed), 5)
    sources = gaussian(seeds[0], (N_ROW, N_COL, LEAF, RHS), 1.0, 6.0, ((0, 8), (1, 4)), jnp.float32)
    leaf_basis = gaussian(seeds[1], (N_ROW, N_COL, LEAF, RANK), LEAF ** -0.5, 0.25, ((0, 8), (1, 4)), jnp.float32)
    transfers = gaussian(seeds[2], (N_ROW, N_COL, LEVELS, RANK, 2 * RANK), (2 * RANK) ** -0.5, 0.25, ((0, 8), (1, 4)), jnp.float32)
    out_basis = gaussian(seeds[3], (N_ROW, N_COL, LEAF, RANK), RANK ** -0.5, 0.375, ((0, 8), (1, 4)), jnp.float32)
    return {"sources": sources, "leaf_basis": leaf_basis, "transfers": transfers, "out_basis": out_basis}


def partner(coeff, axis, bit):
    span = 1 << bit
    shape = coeff.shape
    if axis == 0:
        split = coeff.reshape((shape[0] // (2 * span), 2, span) + shape[1:])
        return jnp.flip(split, 1).reshape(shape)
    split = coeff.reshape((shape[0], shape[1] // (2 * span), 2, span) + shape[2:])
    return jnp.flip(split, 2).reshape(shape)


def reference(sources, leaf_basis, transfers, out_basis):
    high = lax.Precision.HIGHEST
    coeff = jnp.einsum("abmk,abmr->abkr", leaf_basis, sources, precision=high)
    row_bits = N_ROW.bit_length() - 1
    col_bits = N_COL.bit_length() - 1
    for level in range(LEVELS):
        if level % 2 == 0:
            other = partner(coeff, 0, row_bits - 1 - level // 2)
        else:
            other = partner(coeff, 1, col_bits - 1 - level // 2)
        block = transfers[:, :, level]
        coeff = jnp.einsum("abkj,abjr->abkr", block[..., :RANK], coeff, precision=high) + jnp.einsum("abkj,abjr->abkr", block[..., RANK:], other, precision=high)
    return jnp.einsum("abmk,abkr->abmr", out_basis, coeff, precision=high)
```

```python
import jax
import jax.numpy as jnp
from jax import lax
from jax.experimental import pallas as pl
from jax.experimental.pallas import tpu as pltpu
from jax.sharding import PartitionSpec as P

GROUP = 128
CHUNK = 64
LAGS = (0, 256, 384, 576)
RAMP = (32, 32, 64)
LIMIT = 8 * 2**20


def split(x):
    high = x.astype(jnp.bfloat16)
    return high, (x - high.astype(jnp.float32)).astype(jnp.bfloat16)


def product(left, right_high, right_low, right_dim):
    dims = (((1,), (right_dim,)), ((), ()))
    rows = left.shape[0]
    high, low = split(left)
    both = lax.dot_general(
        jnp.concatenate([high, low], axis=0), right_high, dims, preferred_element_type=jnp.float32
    )
    rest = lax.dot_general(high, right_low, dims, preferred_element_type=jnp.float32)
    return both[:rows] + (both[rows:] + rest)


def chunks_of(rhs):
    body = rhs - 2 * sum(RAMP)
    sizes = list(RAMP) + [CHUNK] * (body // CHUNK)
    if body % CHUNK:
        sizes.append(body % CHUNK)
    sizes += list(RAMP)[::-1]
    starts = [sum(sizes[:at]) for at in range(len(sizes))]
    return list(zip(starts, sizes))


def order_of(chunks, levels):
    steps = []
    for at, (start, size) in enumerate(chunks):
        for level in range(levels):
            steps.append((start + LAGS[level], -level, at, level))
    return [(at, -low) for _, low, at, _ in sorted(steps)]


def partner(level, levels):
    axis = "row" if level % 2 == 0 else "col"
    span = lax.axis_size(axis) >> (1 + level // 2)
    me = lax.axis_index(axis)
    return {axis: me + span - 2 * span * ((me // span) % 2)}


def kernel(
    src, leaf, tra, outb, res,
    src_v, leaf_v, tra_v, outb_v, coeff, other, t_high, t_low, o_both,
    in_sem, tra_sem, send_sem, recv_sem,
):
    levels, rank = tra.shape[0], leaf.shape[1]
    rhs = src.shape[1]
    groups = rhs // GROUP
    chunks = chunks_of(rhs)
    partners = [partner(level, levels) for level in range(levels)]

    barrier = pltpu.get_barrier_semaphore()
    for who in partners:
        pl.semaphore_signal(barrier, inc=1, device_id=who, device_id_type=pl.DeviceIdType.MESH)

    load_leaf = pltpu.make_async_copy(leaf, leaf_v, in_sem.at[groups])
    load_leaf.start()
    load_src = []
    for g in range(groups):
        cols = pl.ds(g * GROUP, GROUP)
        load_src.append(pltpu.make_async_copy(src.at[:, cols], src_v.at[:, cols], in_sem.at[g]))
        load_src[-1].start()
    load_tra = [pltpu.make_async_copy(tra.at[k], tra_v.at[k], tra_sem.at[k]) for k in range(levels)]
    for copy in load_tra:
        copy.start()
    load_outb = pltpu.make_async_copy(outb, outb_v, in_sem.at[groups + 1])
    load_outb.start()

    copies = {}

    def send(at, level):
        rows = pl.ds(*chunks[at])
        copy = pltpu.make_async_remote_copy(
            src_ref=coeff.at[level, rows],
            dst_ref=other.at[level, rows],
            send_sem=send_sem.at[level, at],
            recv_sem=recv_sem.at[level, at],
            device_id=partners[level],
            device_id_type=pl.DeviceIdType.MESH,
        )
        copy.start()
        copies[at, level] = copy

    load_leaf.wait()
    l_high, l_low = split(leaf_v[...])
    for g in range(groups):
        load_src[g].wait()
        turned = src_v[:, g * GROUP:(g + 1) * GROUP].T
        coeff[0, pl.ds(g * GROUP, GROUP), :] = product(turned, l_high, l_low, 0)
        if g == 0:
            pl.semaphore_wait(barrier, levels)
        for at, (start, size) in enumerate(chunks):
            if g * GROUP < start + size <= (g + 1) * GROUP:
                send(at, 0)
    def prepare(k):
        load_tra[k].wait()
        high, low = split(tra_v[k].T)
        t_high[k] = high
        t_low[k] = low

    def mix(k, left, half):
        part = slice(half * rank, (half + 1) * rank)
        return product(left, t_high[k, part, :], t_low[k, part, :], 0)

    def expand(g):
        high, low = split(coeff[levels, pl.ds(g * GROUP, GROUP), :])
        dims = (((1,), (1,)), ((), ()))
        wide = lax.dot_general(o_both[...], high, dims, preferred_element_type=jnp.float32)
        rest = lax.dot_general(o_both[:size, :], low, dims, preferred_element_type=jnp.float32)
        res[:, g * GROUP:(g + 1) * GROUP] = wide[:size] + (wide[size:] + rest)

    prepared = 0
    size = outb.shape[0]
    ready = 0
    missing = [sum(1 for start, n in chunks if start // GROUP == g) for g in range(groups)]
    for at, level in order_of(chunks, levels):
        rows = pl.ds(*chunks[at])
        if level == prepared:
            prepare(level)
            prepared += 1
        own = mix(level, coeff[level, rows, :], 0)
        with jax.named_scope(f"w{level}_{at}"):
            copies[at, level].wait_recv()
        fresh = own + mix(level, other[level, rows, :], 1)
        coeff[level + 1, rows, :] = fresh
        if level + 1 < levels:
            send(at, level + 1)
            continue
        g = chunks[at][0] // GROUP
        missing[g] -= 1
        if ready == 0:
            load_outb.wait()
            high, low = split(outb_v[...])
            o_both[:size, :] = high
            o_both[size:, :] = low
            ready = 1
        if missing[g] == 0:
            expand(g)
    for copy in copies.values():
        copy.wait_send()


def store(held, res, sem):
    groups = sem.shape[0]
    wide = held.shape[0] // groups
    moves = []
    for g in range(groups):
        rows = pl.ds(g * wide, wide)
        moves.append(pltpu.make_async_copy(held.at[rows], res.at[rows], sem.at[g]))
        moves[-1].start()
    for move in moves:
        move.wait()


def body(sources, leaf_basis, transfers, out_basis):
    src, leaf, tra, outb = sources[0, 0], leaf_basis[0, 0], transfers[0, 0], out_basis[0, 0]
    size, rhs = src.shape
    rank = leaf.shape[1]
    count = len(chunks_of(rhs))
    levels = tra.shape[0]
    f32 = jnp.float32
    any_space = pl.BlockSpec(memory_space=pl.ANY)
    hbm = pl.BlockSpec(memory_space=pltpu.HBM)
    held = pl.pallas_call(
        kernel,
        out_shape=pltpu.VMEM((size, rhs), f32),
        in_specs=[hbm] * 4,
        out_specs=pl.BlockSpec(memory_space=pltpu.VMEM),
        scratch_shapes=[
            pltpu.VMEM((size, rhs), f32),
            pltpu.VMEM((size, rank), f32),
            pltpu.VMEM(tra.shape, f32),
            pltpu.VMEM((size, rank), f32),
            pltpu.VMEM((levels + 1, rhs, rank), f32),
            pltpu.VMEM((levels, rhs, rank), f32),
            pltpu.VMEM((levels, 2 * rank, rank), jnp.bfloat16),
            pltpu.VMEM((levels, 2 * rank, rank), jnp.bfloat16),
            pltpu.VMEM((2 * size, rank), jnp.bfloat16),
            pltpu.SemaphoreType.DMA((rhs // GROUP + 2,)),
            pltpu.SemaphoreType.DMA((levels,)),
            pltpu.SemaphoreType.DMA((levels, count)),
            pltpu.SemaphoreType.DMA((levels, count)),
        ],
        compiler_params=pltpu.CompilerParams(
            collective_id=0, has_side_effects=True
        ),
    )(src, leaf, tra, outb)
    result = pl.pallas_call(
        store,
        out_shape=jax.ShapeDtypeStruct((size, rhs), f32),
        in_specs=[pl.BlockSpec(memory_space=pltpu.VMEM)],
        out_specs=any_space,
        scratch_shapes=[pltpu.SemaphoreType.DMA((4,))],
        compiler_params=pltpu.CompilerParams(vmem_limit_bytes=LIMIT),
    )(held)
    return result[None, None]


def solution(mesh):
    in_specs = (
        P("row", "col", None, None),
        P("row", "col", None, None),
        P("row", "col", None, None, None),
        P("row", "col", None, None),
    )
    out_specs = P("row", "col", None, None)
    return jax.shard_map(body, mesh=mesh, in_specs=in_specs, out_specs=out_specs, check_vma=False)
```

```python
import jax
import jax.numpy as jnp
from jax import lax
from jax.experimental import pallas as pl
from jax.experimental.pallas import tpu as pltpu
from jax.sharding import PartitionSpec as P

GROUP = 128
CHUNK = 64
FIRST = 128
LAGS = ((0, 240, 416, 672, 592), (0, 240, 256, 512, 496))
SLOPES = ((1, 1, 1, 1, 1.2), (1, 0.8, 1, 0.9, 1.0))
HEAD = (32, 32, 64)
TAIL = (64, 32, 32)
LIMIT = 8 * 2**20


def split(x):
    high = x.astype(jnp.bfloat16)
    return high, (x - high.astype(jnp.float32)).astype(jnp.bfloat16)


def product(left, right_high, right_low, right_dim):
    dims = (((1,), (right_dim,)), ((), ()))
    rows = left.shape[0]
    high, low = split(left)
    both = lax.dot_general(
        jnp.concatenate([high, low], axis=0), right_high, dims, preferred_element_type=jnp.float32
    )
    rest = lax.dot_general(high, right_low, dims, preferred_element_type=jnp.float32)
    return both[:rows] + (both[rows:] + rest)


def chunks_of(rhs):
    body = rhs - sum(HEAD) - sum(TAIL)
    sizes = list(HEAD) + [CHUNK] * (body // CHUNK)
    if body % CHUNK:
        sizes.append(body % CHUNK)
    sizes += list(TAIL)
    starts = [sum(sizes[:at]) for at in range(len(sizes))]
    return list(zip(starts, sizes))


def order_of(chunks, levels, lags, slopes):
    steps = []
    groups = chunks[-1][0] // GROUP + 1
    for at, (start, size) in enumerate(chunks):
        last = (start + size) % GROUP == 0 and start // GROUP + 1 < groups
        for level in range(levels + last):
            key = start * slopes[level] + lags[level]
            if level:
                key = max(key, steps[-1][0] + 1)
            steps.append((key, -level, at, level))
    return [(at, level) for _, _, at, level in sorted(steps)]


def expand(o_both, coeff):
    size = o_both.shape[0] // 2
    high, low = split(coeff)
    dims = (((1,), (1,)), ((), ()))
    wide = lax.dot_general(o_both[...], high, dims, preferred_element_type=jnp.float32)
    rest = lax.dot_general(o_both[:size, :], low, dims, preferred_element_type=jnp.float32)
    return wide[:size] + (wide[size:] + rest)


def partner(level, levels):
    axis = "row" if level % 2 == 0 else "col"
    span = lax.axis_size(axis) >> (1 + level // 2)
    me = lax.axis_index(axis)
    return {axis: me + span - 2 * span * ((me // span) % 2)}


def kernel(
    src, leaf, tra, outb, held, tail, o_both,
    src_v, leaf_v, tra_v, outb_v, coeff, other, t_high, t_low,
    in_sem, send_sem, recv_sem,
):
    levels, rank = tra.shape[0], leaf.shape[1]
    rhs = src.shape[1]
    groups = rhs // GROUP
    chunks = chunks_of(rhs)
    partners = [partner(level, levels) for level in range(levels)]

    barrier = pltpu.get_barrier_semaphore()
    for who in partners:
        pl.semaphore_signal(barrier, inc=1, device_id=who, device_id_type=pl.DeviceIdType.MESH)

    load_leaf = pltpu.make_async_copy(leaf, leaf_v, in_sem.at[0])
    load_leaf.start()
    load_src = []
    for at, cols in enumerate((pl.ds(0, GROUP), pl.ds(GROUP, rhs - GROUP))):
        load_src.append(pltpu.make_async_copy(src.at[:, cols], src_v.at[:, cols], in_sem.at[1 + at]))
        load_src[-1].start()
    load_tra = [
        pltpu.make_async_copy(tra.at[ks], tra_v.at[ks], in_sem.at[3 + at])
        for at, ks in enumerate((pl.ds(0, 1), pl.ds(1, levels - 1)))
    ]
    load_outb = pltpu.make_async_copy(outb, outb_v, in_sem.at[5])

    def copy_of(at, level):
        rows = pl.ds(*chunks[at])
        return pltpu.make_async_remote_copy(
            src_ref=coeff.at[level, rows],
            dst_ref=other.at[level, rows],
            send_sem=send_sem.at[0],
            recv_sem=recv_sem.at[level, at],
            device_id=partners[level],
            device_id_type=pl.DeviceIdType.MESH,
        )

    load_leaf.wait()
    l_high, l_low = split(leaf_v[...])
    for g in range(groups):
        if g < 2:
            load_src[g].wait()
        if g == 0:
            for copy in load_tra:
                copy.start()
            load_outb.start()
        turned = src_v[:, g * GROUP:(g + 1) * GROUP].T
        edges = (0, FIRST, GROUP) if g == 0 and FIRST < GROUP else (0, GROUP)
        for low, high in zip(edges[:-1], edges[1:]):
            rows = pl.ds(g * GROUP + low, high - low)
            coeff[0, rows, :] = product(turned[low:high], l_high, l_low, 0)
            if g + low == 0:
                pl.semaphore_wait(barrier, levels)
            for at, (start, size) in enumerate(chunks):
                if g * GROUP + low < start + size <= g * GROUP + high:
                    copy_of(at, 0).start()

    def prepare(k):
        if k < 2:
            load_tra[k].wait()
        if k == levels:
            load_outb.wait()
            high, low = split(outb_v[...])
            o_both[:size, :] = high
            o_both[size:, :] = low
            return
        high, low = split(tra_v[k].T)
        t_high[k] = high
        t_low[k] = low

    def mix(k, left, half):
        part = slice(half * rank, (half + 1) * rank)
        return product(left, t_high[k, part, :], t_low[k, part, :], 0)

    size = outb.shape[0]

    body_cols = rhs - tail.shape[0]

    def run(order):
        prepared = 0
        for step, (at, level) in enumerate(order):
            start, count = chunks[at]
            rows = pl.ds(start, count)
            if level == levels:
                cols = pl.ds(start // GROUP * GROUP, GROUP)
                with jax.named_scope(f"x{at}"):
                    held[:, cols] = expand(o_both, coeff[levels, cols, :])
                continue
            while prepared <= levels and (step >= prepared or level >= prepared):
                prepare(prepared)
                prepared += 1
            own = mix(level, coeff[level, rows, :], 0)
            with jax.named_scope(f"w{level}_{at}"):
                copy_of(at, level).wait_recv()
            fresh = own + mix(level, other[level, rows, :], 1)
            if level + 1 < levels:
                coeff[level + 1, rows, :] = fresh
                copy_of(at, level + 1).start()
            elif start < body_cols:
                coeff[levels, rows, :] = fresh
            else:
                tail[pl.ds(start - body_cols, count), :] = fresh

    core = lax.axis_index("row") % 2
    orders = [order_of(chunks, levels, *pair) for pair in zip(LAGS, SLOPES)]
    if orders[0] == orders[1]:
        run(orders[0])
    else:
        for k in range(2):
            pl.when(core == k)(lambda k=k: run(orders[k]))
    with jax.named_scope("end"):
        pltpu.make_async_remote_copy(
            src_ref=coeff.at[pl.ds(0, levels)],
            dst_ref=other,
            send_sem=send_sem.at[0],
            recv_sem=recv_sem.at[0, 0],
            device_id=partners[0],
            device_id_type=pl.DeviceIdType.MESH,
        ).wait_send()


def store(held, tail, o_both, res, last, sem):
    done = held.shape[1]
    early = pltpu.make_async_copy(held, res.at[:, pl.ds(0, done)], sem.at[0])
    early.start()
    last[...] = expand(o_both, tail[...])
    late = pltpu.make_async_copy(last, res.at[:, pl.ds(done, last.shape[1])], sem.at[1])
    late.start()
    early.wait()
    late.wait()


def body(sources, leaf_basis, transfers, out_basis):
    src, leaf, tra, outb = sources[0, 0], leaf_basis[0, 0], transfers[0, 0], out_basis[0, 0]
    size, rhs = src.shape
    rank = leaf.shape[1]
    count = len(chunks_of(rhs))
    levels = tra.shape[0]
    f32 = jnp.float32
    any_space = pl.BlockSpec(memory_space=pl.ANY)
    hbm = pl.BlockSpec(memory_space=pltpu.HBM)
    vmem = pl.BlockSpec(memory_space=pltpu.VMEM)
    parts = pl.pallas_call(
        kernel,
        out_shape=[
            pltpu.VMEM((size, rhs - GROUP), f32),
            pltpu.VMEM((GROUP, rank), f32),
            pltpu.VMEM((2 * size, rank), jnp.bfloat16),
        ],
        in_specs=[hbm] * 4,
        out_specs=[vmem] * 3,
        scratch_shapes=[
            pltpu.VMEM((size, rhs), f32),
            pltpu.VMEM((size, rank), f32),
            pltpu.VMEM(tra.shape, f32),
            pltpu.VMEM((size, rank), f32),
            pltpu.VMEM((levels + 1, rhs, rank), f32),
            pltpu.VMEM((levels, rhs, rank), f32),
            pltpu.VMEM((levels, 2 * rank, rank), jnp.bfloat16),
            pltpu.VMEM((levels, 2 * rank, rank), jnp.bfloat16),
            pltpu.SemaphoreType.DMA((6,)),
            pltpu.SemaphoreType.DMA((1,)),
            pltpu.SemaphoreType.DMA((levels, count)),
        ],
        compiler_params=pltpu.CompilerParams(
            collective_id=0, has_side_effects=True
        ),
    )(src, leaf, tra, outb)
    result = pl.pallas_call(
        store,
        out_shape=jax.ShapeDtypeStruct((size, rhs), f32),
        in_specs=[vmem] * 3,
        out_specs=any_space,
        scratch_shapes=[pltpu.VMEM((size, GROUP), f32), pltpu.SemaphoreType.DMA((2,))],
        compiler_params=pltpu.CompilerParams(vmem_limit_bytes=LIMIT),
    )(*parts)
    return result[None, None]


def solution(mesh):
    in_specs = (
        P("row", "col", None, None),
        P("row", "col", None, None),
        P("row", "col", None, None, None),
        P("row", "col", None, None),
    )
    out_specs = P("row", "col", None, None)
    return jax.shard_map(body, mesh=mesh, in_specs=in_specs, out_specs=out_specs, check_vma=False)
```

```python
import jax
import jax.numpy as jnp
from jax import lax
from jax.experimental import pallas as pl
from jax.experimental.pallas import tpu as pltpu
from jax.sharding import PartitionSpec as P

GROUP = 128
CHUNK = 64
FIRST = 64
EARLY = 1
LAGS = ((0, 240, 416, 672, 720), (0, 240, 256, 512, 496))
SLOPES = ((1, 1, 1, 1, 1.2), (1, 0.8, 1, 0.9, 1.0))
HEAD = (32, 32, 64)
TAIL = (64, 40, 24)
LIMIT = 8 * 2**20


def split(x):
    high = x.astype(jnp.bfloat16)
    return high, (x - high.astype(jnp.float32)).astype(jnp.bfloat16)


def product(left, right_high, right_low, right_dim):
    dims = (((1,), (right_dim,)), ((), ()))
    rows = left.shape[0]
    high, low = split(left)
    both = lax.dot_general(
        jnp.concatenate([high, low], axis=0), right_high, dims, preferred_element_type=jnp.float32
    )
    rest = lax.dot_general(high, right_low, dims, preferred_element_type=jnp.float32)
    return both[:rows] + (both[rows:] + rest)


def chunks_of(rhs):
    body = rhs - sum(HEAD) - sum(TAIL)
    sizes = list(HEAD) + [CHUNK] * (body // CHUNK)
    if body % CHUNK:
        sizes.append(body % CHUNK)
    sizes += list(TAIL)
    starts = [sum(sizes[:at]) for at in range(len(sizes))]
    return list(zip(starts, sizes))


def order_of(chunks, levels, lags, slopes):
    steps = []
    groups = chunks[-1][0] // GROUP + 1
    for at, (start, size) in enumerate(chunks):
        last = (start + size) % GROUP == 0 and start // GROUP + 1 < groups
        for level in range(levels + last):
            key = start * slopes[level] + lags[level]
            if level:
                key = max(key, steps[-1][0] + 1)
            steps.append((key, -level, at, level))
    return [(at, level) for _, _, at, level in sorted(steps)]


def expand(o_cat, coeff):
    high, low = split(coeff)
    both = jnp.concatenate([high, low, high], axis=1)
    dims = (((1,), (1,)), ((), ()))
    return lax.dot_general(o_cat[...], both, dims, preferred_element_type=jnp.float32)


def partner(level, levels):
    axis = "row" if level % 2 == 0 else "col"
    span = lax.axis_size(axis) >> (1 + level // 2)
    me = lax.axis_index(axis)
    return {axis: me + span - 2 * span * ((me // span) % 2)}


def kernel(
    src, leaf, tra, outb, held, tail, o_cat,
    src_v, leaf_v, tra_v, outb_v, coeff, other, t_high, t_low,
    in_sem, send_sem, recv_sem,
):
    levels, rank = tra.shape[0], leaf.shape[1]
    rhs = src.shape[1]
    groups = rhs // GROUP
    chunks = chunks_of(rhs)
    partners = [partner(level, levels) for level in range(levels)]

    barrier = pltpu.get_barrier_semaphore()
    for who in partners:
        pl.semaphore_signal(barrier, inc=1, device_id=who, device_id_type=pl.DeviceIdType.MESH)

    load_leaf = pltpu.make_async_copy(leaf, leaf_v, in_sem.at[0])
    load_leaf.start()
    load_src = []
    for at, cols in enumerate((pl.ds(0, GROUP), pl.ds(GROUP, rhs - GROUP))):
        load_src.append(pltpu.make_async_copy(src.at[:, cols], src_v.at[:, cols], in_sem.at[1 + at]))
        load_src[-1].start()
    load_tra = [
        pltpu.make_async_copy(tra.at[ks], tra_v.at[ks], in_sem.at[3 + at])
        for at, ks in enumerate((pl.ds(0, 1), pl.ds(1, levels - 1)))
    ]
    load_outb = pltpu.make_async_copy(outb, outb_v, in_sem.at[5])

    def copy_of(at, level):
        rows = pl.ds(*chunks[at])
        return pltpu.make_async_remote_copy(
            src_ref=coeff.at[level, rows],
            dst_ref=other.at[level, rows],
            send_sem=send_sem.at[0],
            recv_sem=recv_sem.at[level, at],
            device_id=partners[level],
            device_id_type=pl.DeviceIdType.MESH,
        )

    load_leaf.wait()
    l_high, l_low = split(leaf_v[...])
    for g in range(groups):
        if g < 2:
            load_src[g].wait()
        if g == 0:
            for copy in load_tra:
                copy.start()
            load_outb.start()
        turned = src_v[:, g * GROUP:(g + 1) * GROUP].T
        edges = (0, FIRST, GROUP) if g == 0 and FIRST < GROUP else (0, GROUP)
        for low, high in zip(edges[:-1], edges[1:]):
            rows = pl.ds(g * GROUP + low, high - low)
            coeff[0, rows, :] = product(turned[low:high], l_high, l_low, 0)
            if g + low == 0:
                pl.semaphore_wait(barrier, levels)
            for at, (start, size) in enumerate(chunks):
                if g * GROUP + low < start + size <= g * GROUP + high:
                    copy_of(at, 0).start()

    def prepare(k):
        if k < 2:
            load_tra[k].wait()
        if k == levels:
            load_outb.wait()
            high, low = split(outb_v[...])
            o_cat[:, :rank] = high
            o_cat[:, rank:2 * rank] = high
            o_cat[:, 2 * rank:] = low
            return
        high, low = split(tra_v[k].T)
        t_high[k] = high
        t_low[k] = low

    def mix(k, left, half):
        part = slice(half * rank, (half + 1) * rank)
        return product(left, t_high[k, part, :], t_low[k, part, :], 0)

    size = outb.shape[0]

    body_cols = rhs - tail.shape[0]

    def run(order):
        prepared = 0
        for step, (at, level) in enumerate(order):
            start, count = chunks[at]
            rows = pl.ds(start, count)
            if level == levels:
                cols = pl.ds(start // GROUP * GROUP, GROUP)
                with jax.named_scope(f"x{at}"):
                    held[:, cols] = expand(o_cat, coeff[levels, cols, :])
                continue
            while prepared <= levels and (step >= prepared or level >= prepared):
                prepare(prepared)
                prepared += 1
            own = mix(level, coeff[level, rows, :], 0)
            with jax.named_scope(f"w{level}_{at}"):
                copy_of(at, level).wait_recv()
            fresh = own + mix(level, other[level, rows, :], 1)
            if level + 1 < levels:
                coeff[level + 1, rows, :] = fresh
                copy_of(at, level + 1).start()
            elif start < body_cols:
                coeff[levels, rows, :] = fresh
            else:
                tail[pl.ds(start - body_cols, count), :] = fresh

    core = lax.axis_index("row") % 2
    orders = [order_of(chunks, levels, *pair) for pair in zip(LAGS, SLOPES)]
    if orders[0] == orders[1]:
        run(orders[0])
    else:
        for k in range(2):
            pl.when(core == k)(lambda k=k: run(orders[k]))
    with jax.named_scope("end"):
        pltpu.make_async_remote_copy(
            src_ref=coeff.at[pl.ds(0, levels)],
            dst_ref=other,
            send_sem=send_sem.at[0],
            recv_sem=recv_sem.at[0, 0],
            device_id=partners[0],
            device_id_type=pl.DeviceIdType.MESH,
        ).wait_send()


def store(held, tail, o_cat, res, last, sem):
    done = held.shape[1]
    part = held.shape[0] // EARLY
    early = []
    for at in range(EARLY):
        rows = pl.ds(at * part, part)
        early.append(pltpu.make_async_copy(held.at[rows], res.at[rows, pl.ds(0, done)], sem.at[1 + at]))
        early[-1].start()
    last[...] = expand(o_cat, tail[...])
    late = pltpu.make_async_copy(last, res.at[:, pl.ds(done, last.shape[1])], sem.at[0])
    late.start()
    for copy in early:
        copy.wait()
    late.wait()


def body(sources, leaf_basis, transfers, out_basis):
    src, leaf, tra, outb = sources[0, 0], leaf_basis[0, 0], transfers[0, 0], out_basis[0, 0]
    size, rhs = src.shape
    rank = leaf.shape[1]
    count = len(chunks_of(rhs))
    levels = tra.shape[0]
    f32 = jnp.float32
    any_space = pl.BlockSpec(memory_space=pl.ANY)
    hbm = pl.BlockSpec(memory_space=pltpu.HBM)
    vmem = pl.BlockSpec(memory_space=pltpu.VMEM)
    parts = pl.pallas_call(
        kernel,
        out_shape=[
            pltpu.VMEM((size, rhs - GROUP), f32),
            pltpu.VMEM((GROUP, rank), f32),
            pltpu.VMEM((size, 3 * rank), jnp.bfloat16),
        ],
        in_specs=[hbm] * 4,
        out_specs=[vmem] * 3,
        scratch_shapes=[
            pltpu.VMEM((size, rhs), f32),
            pltpu.VMEM((size, rank), f32),
            pltpu.VMEM(tra.shape, f32),
            pltpu.VMEM((size, rank), f32),
            pltpu.VMEM((levels + 1, rhs, rank), f32),
            pltpu.VMEM((levels, rhs, rank), f32),
            pltpu.VMEM((levels, 2 * rank, rank), jnp.bfloat16),
            pltpu.VMEM((levels, 2 * rank, rank), jnp.bfloat16),
            pltpu.SemaphoreType.DMA((6,)),
            pltpu.SemaphoreType.DMA((1,)),
            pltpu.SemaphoreType.DMA((levels, count)),
        ],
        compiler_params=pltpu.CompilerParams(
            collective_id=0, has_side_effects=True
        ),
    )(src, leaf, tra, outb)
    result = pl.pallas_call(
        store,
        out_shape=jax.ShapeDtypeStruct((size, rhs), f32),
        in_specs=[vmem] * 3,
        out_specs=any_space,
        scratch_shapes=[pltpu.VMEM((size, GROUP), f32), pltpu.SemaphoreType.DMA((1 + EARLY,))],
        compiler_params=pltpu.CompilerParams(vmem_limit_bytes=LIMIT),
    )(*parts)
    return result[None, None]


def solution(mesh):
    in_specs = (
        P("row", "col", None, None),
        P("row", "col", None, None),
        P("row", "col", None, None, None),
        P("row", "col", None, None),
    )
    out_specs = P("row", "col", None, None)
    return jax.shard_map(body, mesh=mesh, in_specs=in_specs, out_specs=out_specs, check_vma=False)
```
